32 devices in a mesh: section: 4 (over x, core), shard: 2 (over y), replica: 4 (over z).
Axes of the slice: x: 2, y: 2, z: 4, core: 2. Of those that a mesh axis runs over, the one named last changes fastest.
Arguments:
- acts_fwd: bfloat16 [4, 1024, 4096], P('section', ('shard', 'replica')), may hold values from -30 to 30
- pos_fwd: int32 [4, 1024], P('section', ('shard', 'replica')), may hold values from 0 to 2047
- saved_acts: bfloat16 [4, 1024, 4096], P('section', ('shard', 'replica')), may hold values from -30 to 30
- pos_bwd: int32 [4, 1024], P('section', ('shard', 'replica')), may hold values from 0 to 2047
- grads_in: bfloat16 [4, 1024, 4096], P('section', ('shard', 'replica')), may hold values from -6 to 6
- key_cotan: bfloat16 [4, 1024, 512], P('section', ('shard', 'replica')), may hold values from -6 to 6
- weight: bfloat16 [4, 4096, 512], P('section', 'shard'), may hold values from -0.09375 to 0.09375
- gain: float32 [4, 4096], P('section'), may hold values from 0.1 to 1.9
Outputs:
- keys: bfloat16 [4, 1024, 512], P('section', ('shard', 'replica'))
- grad_out: bfloat16 [4, 1024, 4096], P('section', ('shard', 'replica'))
- weight_grad: float32 [4, 4096, 512], P('section', 'shard')
The draws below stay inside these ranges and needn't reach their ends.
All inputs are finite; a program needn't handle non-finite values.
Results may differ from the reference program's by a relative error of at most 0.0058.
Values may be sent and summed in bfloat16 or wider, within the bound.
A program may use at most 64 MiB of HBM per device.

```python
import math
import jax
import jax.numpy as jnp
from jax import lax

D = 4096
HEAD = 128
KVH = 4
SEQ = 2048
TOK_DEV = 128
TOKENS = 1024
N_SECTION = 4


def rough_rows(key):
    shape = (N_SECTION, TOKENS, D)
    scale_key = jax.random.fold_in(key, 11)
    base_key = jax.random.fold_in(key, 12)
    scales = jnp.exp(jax.random.uniform(scale_key, (N_SECTION, TOKENS, 1), jnp.float32, math.log(0.5), math.log(5.0)))
    base = jnp.clip(jax.random.normal(base_key, shape, jnp.float32), -5.0, 5.0)
    values = base * scales
    return jnp.clip(values, -30.0, 30.0).astype(jnp.bfloat16)


def draw_acts_fwd(key, part):
    return rough_rows(jax.random.fold_in(key, 101))


def draw_saved_acts(key, part):
    return rough_rows(jax.random.fold_in(key, 202))


def plant(entries, own_key, smallest, top_value):
    shape = entries.shape
    index_at = [jax.random.randint(jax.random.fold_in(own_key, axis), (), 0, shape[axis]) for axis in range(len(shape))]
    entries = entries.at[tuple(index_at)].set(smallest)
    longest = shape.index(max(shape))
    index_at[longest] = (index_at[longest] + 1) % shape[longest]
    return entries.at[tuple(index_at)].set(top_value)


def levels(key, shape, pieces, low, largest):
    def one(axis_at, shards_of):
        heights = jax.random.uniform(jax.random.fold_in(jax.random.fold_in(key, 6), axis_at), (shards_of,), jnp.float32, low / len(pieces), largest / len(pieces))
        return jnp.repeat(jnp.exp(heights), shape[axis_at] // shards_of).reshape((-1,) + (1,) * (len(shape) - axis_at - 1))

    factor_of = one(*pieces[0])
    for cut in pieces[1:]:
        factor_of = factor_of * one(*cut)
    return factor_of


def noise(own_key, extent, width, limit, split=(), kind=jnp.bfloat16):
    values = width * jax.random.normal(own_key, extent, jnp.float32)
    if split:
        values = values * levels(own_key, extent, split, -0.22, 0.18)
    return jnp.clip(values, -limit, limit).astype(kind)


def setup_inputs(seed: int = 0) -> dict:
    key_list = jax.random.split(jax.random.key(seed), 9)
    acts_fwd = draw_acts_fwd(jax.random.fold_in(key_list[8], 71), 0)
    pos_fwd = plant(jax.random.randint(key_list[1], (N_SECTION, TOKENS), 0, SEQ), jax.random.fold_in(key_list[1], 1), 0, SEQ - 1).astype(jnp.int32)
    saved_acts = draw_saved_acts(jax.random.fold_in(key_list[8], 71), 0)
    pos_bwd = plant(jax.random.randint(key_list[3], (N_SECTION, TOKENS), 0, SEQ), jax.random.fold_in(key_list[3], 1), 0, SEQ - 1).astype(jnp.int32)
    grads_in = noise(key_list[4], (N_SECTION, TOKENS, D), 1.0, 6.0, ((0, 4), (1, 8)))
    key_cotan = noise(key_list[5], (N_SECTION, TOKENS, KVH * HEAD), 1.0, 6.0, ((0, 4), (1, 8)))
    weight = noise(key_list[6], (N_SECTION, D, KVH * HEAD), D ** -0.5, 0.09375, ((0, 4), (1, 2)))
    gain = jnp.clip(1.0 + 0.18 * jax.random.normal(key_list[7], (N_SECTION, D), jnp.float32), 0.1, 1.9)
    return dict(acts_fwd=acts_fwd, pos_fwd=pos_fwd, saved_acts=saved_acts, pos_bwd=pos_bwd, grads_in=grads_in, key_cotan=key_cotan, weight=weight, gain=gain)


def rope_tables(positions):
    index = jnp.arange(HEAD // 2, dtype=jnp.float32)
    rate = 500000.0 ** (-(2.0 * index) / HEAD)
    angle = positions.astype(jnp.float32)[:, None] * rate[None, :]
    return (jnp.cos(angle), jnp.sin(angle))

def rotate(values, cosine, sine_part, orient):
    count = values.shape[0]
    shaped = values.reshape(count, KVH, HEAD)
    first_half = shaped[..., :HEAD // 2]
    second_half = shaped[..., HEAD // 2:]
    cos_b = cosine[:, None, :]
    sin_b = orient * sine_part[:, None, :]
    joined = jnp.concatenate([first_half * cos_b - second_half * sin_b, second_half * cos_b + first_half * sin_b], -1)
    return joined.reshape(count, KVH * HEAD)

def normalize(stream, gain_row):
    values = stream.astype(jnp.float32)
    inverse = lax.rsqrt(lax.optimization_barrier(jnp.mean(values * values, -1, keepdims=True)) + 1e-05)
    return (values * inverse * gain_row[None, :], inverse, values)

def one_section(packed):
    stream, pos_f, saved, pos_b, arrived, cotan, proj, gain_row = packed
    normed = normalize(stream, gain_row)[0].astype(jnp.bfloat16)
    projected = jnp.dot(normed, proj, preferred_element_type=jnp.float32)
    cosine, sine_part = rope_tables(pos_f)
    keys = rotate(projected, cosine, sine_part, 1.0).astype(jnp.bfloat16)
    back_f, inverse, saved_f = normalize(saved, gain_row)
    back_normed = back_f.astype(jnp.bfloat16)
    cos_b, sin_b = rope_tables(pos_b)
    key_grad = rotate(cotan.astype(jnp.float32), cos_b, sin_b, -1.0).astype(jnp.bfloat16)
    normed_grad = jnp.dot(key_grad, proj.T, preferred_element_type=jnp.float32)
    scaled = normed_grad * gain_row[None, :]
    stream_grad = inverse * scaled - saved_f * inverse ** 3 * lax.optimization_barrier(jnp.mean(saved_f * scaled, -1, keepdims=True))
    grad_out = (arrived.astype(jnp.float32) + stream_grad).astype(jnp.bfloat16)
    blocks = TOKENS // TOK_DEV
    norm_blocks = back_normed.reshape(blocks, TOK_DEV, D)
    grad_blocks = key_grad.reshape(blocks, TOK_DEV, KVH * HEAD)

    def accumulate(total, pair):
        term = lax.dot_general(pair[0], pair[1], (((0,), (0,)), ((), ())), preferred_element_type=jnp.float32)
        rounded = lax.optimization_barrier(term.astype(jnp.bfloat16))
        return (total + rounded.astype(jnp.float32), None)
    start = jnp.zeros((D, KVH * HEAD), jnp.float32)
    total, unused = lax.scan(accumulate, start, (norm_blocks, grad_blocks))
    weight_grad = total * float(TOKENS) ** (-0.5)
    return (keys, grad_out, weight_grad)

def reference(acts_fwd, pos_fwd, saved_acts, pos_bwd, grads_in, key_cotan, weight, gain):
    streams = jnp.concatenate([acts_fwd[:1], acts_fwd[:-1]], 0)
    arrivals = jnp.concatenate([grads_in[1:], grads_in[-1:]], 0)
    keys, grad_out, weight_grad = lax.map(one_section, (streams, pos_fwd, saved_acts, pos_bwd, arrivals, key_cotan, weight, gain))
    return (keys, grad_out, weight_grad)
```

```python
import functools

import jax
import jax.numpy as jnp
import numpy as np
from jax import lax
from jax.experimental import pallas as pl
from jax.experimental.pallas import tpu as pltpu
from jax.sharding import PartitionSpec as P

HEAD = 128
THETA = 500000.0
EPS = 1e-05
ROWS = 128
PIECES = 4
SKEW = 2
F32 = jnp.float32
BF16 = jnp.bfloat16
MESH = pl.DeviceIdType.MESH


def kernel(
    X, S, R,
    acts, grads, saved, kcot, w, gain, pos_f, pos_b, rate,
    keys_o, grad_o, wg_o,
    saved_v, kcot_v, w_v, stream_v, arrived_v,
    sv_recv, kg_all, st_recv, g_buf, g_send, p_buf, p_send, p_own,
    part, from_l, from_r, to_r, to_l, go_v, keys_v, inv_v, tab_v,
    lsem, acts_ss, acts_rs, grads_sem, sv_ss, sv_rs, kg_ss, kg_rs,
    st_ss, st_rs, g_ss, g_rs, p_ss, p_rs, r_ss, r_rs, l_ss, l_rs, out_sem,
):
    s, j, r = (lax.axis_index(a) for a in ("section", "shard", "replica"))
    T, D = saved.shape
    N = kcot.shape[1]
    Fs = w.shape[0]
    C = Fs // ROWS
    Fp = Fs // PIECES
    travel = to_r.dtype

    def cols(p, width=Fs, off=0):
        return pl.ds(pl.multiple_of(p * Fs + off, 128), width)

    def peer(d):
        return lax.rem(j + d, S)

    load_saved = pltpu.make_async_copy(saved, saved_v, lsem.at[0])
    load_kcot = pltpu.make_async_copy(kcot, kcot_v, lsem.at[1])
    load_w = pltpu.make_async_copy(w, w_v, lsem.at[2])
    load_acts = pltpu.make_async_copy(acts, stream_v, lsem.at[3])
    load_grads = pltpu.make_async_copy(grads, arrived_v, lsem.at[4])
    load_saved.start()
    load_kcot.start()
    load_w.start()
    pl.when(s == 0)(load_acts.start)
    pl.when(s == X - 1)(load_grads.start)

    barrier = pltpu.get_barrier_semaphore()

    def greet(axis, index):
        pl.semaphore_signal(barrier, inc=1, device_id={axis: index}, device_id_type=MESH)

    for d in range(1, S):
        greet("shard", peer(d))
    pl.when(s > 0)(lambda: greet("section", s - 1))
    pl.when(s < X - 1)(lambda: greet("section", s + 1))
    pl.when(r > 0)(lambda: greet("replica", r - 1))
    pl.when(r < R - 1)(lambda: greet("replica", r + 1))
    peers = S - 1
    for cond in (s > 0, s < X - 1, r > 0, r < R - 1):
        peers = peers + jnp.where(cond, 1, 0)
    pl.semaphore_wait(barrier, peers)

    def remote(src, dst, ss, rs, axis, index):
        return pltpu.make_async_remote_copy(
            src_ref=src, dst_ref=dst, send_sem=ss, recv_sem=rs,
            device_id={axis: index}, device_id_type=MESH,
        )

    def sv_copy(d, q):
        return remote(
            saved.at[:, cols(peer(d), Fp, q * Fp)],
            sv_recv.at[S - d, :, pl.ds(q * Fp, Fp)],
            sv_ss.at[d, q], sv_rs.at[S - d, q], "shard", peer(d),
        )

    def sv_wait(slot, q):
        remote(
            saved.at[:, pl.ds(0, Fp)],
            sv_recv.at[slot, :, pl.ds(pl.multiple_of(q * Fp, 128), Fp)],
            sv_ss.at[slot, q], sv_rs.at[slot, q], "shard", peer(slot),
        ).wait_recv()

    def slot_copy(src, dst, ss, rs, d):
        return remote(src.at[d], dst.at[S - d], ss.at[d], rs.at[S - d], "shard", peer(d))

    def slot_wait(src, dst, ss, rs, slot):
        remote(src.at[slot], dst.at[slot], ss.at[slot], rs.at[slot], "shard", peer(slot)).wait_recv()

    def acts_copy(d):
        return remote(
            acts.at[:, cols(peer(d))], stream_v.at[:, cols(peer(d))],
            acts_ss.at[d], acts_rs.at[d], "section", jnp.minimum(s + 1, X - 1),
        )

    grads_copy = remote(
        grads, arrived_v, grads_sem.at[0], grads_sem.at[1], "section", jnp.maximum(s - 1, 0)
    )

    def kg_copy(d):
        return remote(
            kg_all.at[0], kg_all.at[S - d], kg_ss.at[d], kg_rs.at[S - d], "shard", peer(d)
        )

    def st_copy(d):
        return remote(
            stream_v.at[:, cols(peer(d))], st_recv.at[S - d],
            st_ss.at[d], st_rs.at[S - d], "shard", peer(d),
        )

    def right_copy(c):
        return remote(
            to_r.at[c], from_l.at[c], r_ss.at[c], r_rs.at[c], "replica", jnp.minimum(r + 1, R - 1)
        )

    def left_copy(c):
        return remote(
            to_l.at[c], from_r.at[c], l_ss.at[c], l_rs.at[c], "replica", jnp.maximum(r - 1, 0)
        )

    for d in range(1, S):
        sv_copy(d, 0).start()

    @pl.when(s < X - 1)
    def _():
        for d in (*range(1, S), 0):
            acts_copy(d).start()

    @pl.when(s > 0)
    def _():
        grads_copy.start()

    lane = lax.broadcasted_iota(jnp.int32, (T, HEAD), 1)

    def tables(pos):
        angle = jnp.broadcast_to(pos[...].astype(F32), (T, T)).T[:, :1] * rate[...]
        sine = jnp.sin(angle)
        return jnp.cos(angle), jnp.where(lane < HEAD // 2, -sine, sine)

    def inverse_rms(ref):
        total = jnp.zeros((T, 128), F32)
        for c in range(D // 128):
            v = ref[:, c * 128 : (c + 1) * 128].astype(F32)
            total = total + v * v
        return lax.rsqrt(jnp.sum(total, -1, keepdims=True) / D + EPS)

    cos_b, sin_b = tables(pos_b)
    load_saved.wait()
    load_kcot.wait()
    inverse = inverse_rms(saved_v)
    inv_v[...] = jnp.broadcast_to(inverse, inv_v.shape)
    for h in range(N // HEAD):
        head = slice(h * HEAD, (h + 1) * HEAD)
        v = kcot_v[:, head].astype(F32)
        v = v * cos_b - pltpu.roll(v, HEAD // 2, 1) * sin_b
        kg_all[0, :, head] = (v * inverse).astype(BF16)
    for d in range(1, S):
        kg_copy(d).start()
    for q in range(1, PIECES):
        for d in range(1, S):
            sv_copy(d, q).start()

    cos_f, sin_f = tables(pos_f)
    tab_v[0] = cos_f
    tab_v[1] = sin_f
    for d in range(1, S):
        slot_wait(kg_all, kg_all, kg_ss, kg_rs, d)

    def relay():
        pl.when(s == 0)(load_acts.wait)
        for d in range(1, S):
            pl.when(s > 0)(acts_copy(d).wait_recv)
            st_copy(d).start()

    tile = min(512, Fs)

    def backward():
        load_w.wait()

        @pl.loop(0, Fs // tile)
        def _(i):
            at = pl.ds(pl.multiple_of(i * tile, 128), tile)
            m = lax.dot_general(
                kg_all[...].reshape(S * T, N), w_v[at, :], (((1,), (1,)), ((), ())),
                preferred_element_type=F32,
            )
            m = (m * gain[:, cols(j, tile, i * tile)]).astype(BF16)
            g_buf[0, :, at] = m[:T]
            for d in range(1, S):
                g_send[d, :, at] = m[d * T : (d + 1) * T]

        for d in range(1, S):
            slot_copy(g_send, g_buf, g_ss, g_rs, d).start()

    def project(block):
        total = jnp.zeros((T, N), F32)
        for i in range(Fs // tile):
            g = gain[:, cols(j, tile, i * tile)]
            x = (block(i * tile).astype(F32) * g).astype(BF16)
            total = total + jnp.dot(
                x, w_v[i * tile : (i + 1) * tile, :], preferred_element_type=F32
            )
        return total

    def forward_own():
        pl.when(s > 0)(acts_copy(0).wait_recv)
        p_own[...] = project(lambda o: stream_v[:, cols(j, tile, o)])

    def forward_peers():
        for d in range(1, S):
            remote(
                stream_v.at[:, pl.ds(0, Fs)], st_recv.at[d], st_ss.at[d], st_rs.at[d],
                "shard", peer(d),
            ).wait_recv()
            p_send[d] = project(lambda o: st_recv[d, :, o : o + tile]).astype(p_send.dtype)
            slot_copy(p_send, p_buf, p_ss, p_rs, d).start()

    def finish_grad():
        pl.when(s == X - 1)(load_grads.wait)
        pl.when(s < X - 1)(grads_copy.wait_recv)
        for d in range(1, S):
            slot_wait(g_send, g_buf, g_ss, g_rs, d)
        total = jnp.zeros((T, 128), F32)
        for d in range(S):
            for o in range(0, Fs, 128):
                v = saved_v[:, cols(peer(d), 128, o)].astype(F32)
                total = total + v * g_buf[d, :, o : o + 128].astype(F32)
        inv = inv_v[:, :1]
        factor = inv * inv * (jnp.sum(total, -1, keepdims=True) / D)
        for d in range(S):
            for o in range(0, Fs, 128):
                at = cols(peer(d), 128, o)
                v = saved_v[:, at].astype(F32) * factor
                g = arrived_v[:, at].astype(F32) + g_buf[d, :, o : o + 128].astype(F32)
                go_v[:, at] = (g - v).astype(BF16)
        pltpu.make_async_copy(go_v, grad_o, out_sem.at[C]).start()

    def finish_keys():
        inv = inverse_rms(stream_v)
        for d in range(1, S):
            slot_wait(p_send, p_buf, p_ss, p_rs, d)
        for h in range(N // HEAD):
            head = slice(h * HEAD, (h + 1) * HEAD)
            v = p_own[:, head]
            for d in range(1, S):
                v = v + p_buf[d, :, head].astype(F32)
            v = v * inv
            v = v * tab_v[0] + pltpu.roll(v, HEAD // 2, 1) * tab_v[1]
            keys_v[:, head] = v.astype(BF16)
        pltpu.make_async_copy(keys_v, keys_o, out_sem.at[C + 1]).start()

    scale = float(T * S * R) ** -0.5

    def write_out(c):
        return pltpu.make_async_copy(
            part.at[c], wg_o.at[pl.ds(pl.multiple_of(c * ROWS, ROWS), ROWS), :], out_sem.at[c]
        )

    def when_chunk(c, *conds):
        cond = (c >= 0) & (c < C)
        for extra in conds:
            cond = cond & extra
        return pl.when(cond)

    far = SKEW * jnp.maximum(r, R - 1 - r)
    per_piece = C // PIECES
    tasks = {1: relay, 2: backward, 4: forward_own, 7: forward_peers}
    steps = C + SKEW * (R - 1)

    def step(t, carry):
        @pl.when((t < C) & (lax.rem(t, per_piece) == 0))
        def _():
            for d in range(1, S):
                sv_wait(d, t // per_piece)

        @pl.when(t < C)
        def _():
            g = gain[:, cols(j, ROWS, t * ROWS)]
            blocks = [saved_v[:, cols(j, ROWS, t * ROWS)]]
            for d in range(1, S):
                blocks.append(sv_recv[d, :, pl.ds(pl.multiple_of(t * ROWS, 128), ROWS)])
            x = jnp.concatenate([(b.astype(F32) * g).astype(BF16) for b in blocks], 0)
            part[t] = lax.dot_general(
                x, kg_all[...].reshape(S * T, N), (((0,), (0,)), ((), ())),
                preferred_element_type=F32,
            )

        a = t - SKEW * r

        @when_chunk(a, r == 0, r < R - 1)
        def _():
            to_r[a] = part[a].astype(travel)
            right_copy(a).start()

        @when_chunk(a, r > 0)
        def _():
            right_copy(a).wait_recv()

        @when_chunk(a, r > 0, r < R - 1)
        def _():
            to_r[a] = (part[a] + from_l[a].astype(F32)).astype(travel)
            right_copy(a).start()

        b = t - SKEW * (R - 1 - r)

        @when_chunk(b, r == R - 1, r > 0)
        def _():
            to_l[b] = part[b].astype(travel)
            left_copy(b).start()

        @when_chunk(b, r < R - 1)
        def _():
            left_copy(b).wait_recv()

        @when_chunk(b, r < R - 1, r > 0)
        def _():
            to_l[b] = (part[b] + from_r[b].astype(F32)).astype(travel)
            left_copy(b).start()

        f = t - far

        @when_chunk(f, r > 0)
        def _():
            part[f] = part[f] + from_l[f].astype(F32)

        @when_chunk(f, r < R - 1)
        def _():
            part[f] = part[f] + from_r[f].astype(F32)

        @when_chunk(f)
        def _():
            part[f] = part[f] * scale
            write_out(f).start()

        for at, task in tasks.items():
            pl.when(t == min(at, C - 1))(task)
        pl.when(t == min(13, steps - 1))(finish_grad)
        pl.when(t == min(15, steps - 1))(finish_keys)
        return carry

    lax.fori_loop(0, steps, step, 0)

    for d in range(1, S):
        for q in range(PIECES):
            sv_copy(d, q).wait_send()
        kg_copy(d).wait_send()
        st_copy(d).wait_send()
        slot_copy(g_send, g_buf, g_ss, g_rs, d).wait_send()
        slot_copy(p_send, p_buf, p_ss, p_rs, d).wait_send()

    @pl.when(s < X - 1)
    def _():
        for d in range(S):
            acts_copy(d).wait_send()

    @pl.when(s > 0)
    def _():
        grads_copy.wait_send()

    @pl.loop(0, C)
    def _(c):
        pl.when(r < R - 1)(right_copy(c).wait_send)
        pl.when(r > 0)(left_copy(c).wait_send)
        write_out(c).wait()

    pltpu.make_async_copy(go_v, grad_o, out_sem.at[C]).wait()
    pltpu.make_async_copy(keys_v, keys_o, out_sem.at[C + 1]).wait()


def per_device(acts_fwd, pos_fwd, saved_acts, pos_bwd, grads_in, key_cotan, weight, gain):
    X, S, R = (lax.axis_size(a) for a in ("section", "shard", "replica"))
    T, D = acts_fwd.shape[1:]
    Fs, N = weight.shape[1:]
    C = Fs // ROWS
    travel = BF16 if R <= 8 else F32
    index = np.arange(HEAD) % (HEAD // 2)
    rate = jnp.asarray(THETA ** (-(2.0 * index) / HEAD), F32)[None]
    hbm = pl.BlockSpec(memory_space=pl.ANY)
    vmem = pl.BlockSpec(memory_space=pltpu.VMEM)
    dma = pltpu.SemaphoreType.DMA
    keys, grad_out, weight_grad = pl.pallas_call(
        functools.partial(kernel, X, S, R),
        out_shape=(
            jax.ShapeDtypeStruct((T, N), BF16),
            jax.ShapeDtypeStruct((T, D), BF16),
            jax.ShapeDtypeStruct((Fs, N), F32),
        ),
        in_specs=[hbm] * 5 + [vmem] * 4,
        out_specs=(hbm, hbm, hbm),
        scratch_shapes=[
            pltpu.VMEM((T, D), BF16),
            pltpu.VMEM((T, N), BF16),
            pltpu.VMEM((Fs, N), BF16),
            pltpu.VMEM((T, D), BF16),
            pltpu.VMEM((T, D), BF16),
            pltpu.VMEM((S, T, Fs), BF16),
            pltpu.VMEM((S, T, N), BF16),
            pltpu.VMEM((S, T, Fs), BF16),
            pltpu.VMEM((S, T, Fs), BF16),
            pltpu.VMEM((S, T, Fs), BF16),
            pltpu.VMEM((S, T, N), BF16),
            pltpu.VMEM((S, T, N), BF16),
            pltpu.VMEM((T, N), F32),
            pltpu.VMEM((C, ROWS, N), F32),
            pltpu.VMEM((C, ROWS, N), travel),
            pltpu.VMEM((C, ROWS, N), travel),
            pltpu.VMEM((C, ROWS, N), travel),
            pltpu.VMEM((C, ROWS, N), travel),
            pltpu.VMEM((T, D), BF16),
            pltpu.VMEM((T, N), BF16),
            pltpu.VMEM((T, HEAD), F32),
            pltpu.VMEM((2, T, HEAD), F32),
            dma((5,)),
            dma((S,)), dma((S,)), dma((2,)),
            dma((S, PIECES)), dma((S, PIECES)),
            dma((S,)), dma((S,)),
            dma((S,)), dma((S,)),
            dma((S,)), dma((S,)),
            dma((S,)), dma((S,)),
            dma((C,)), dma((C,)), dma((C,)), dma((C,)),
            dma((C + 2,)),
        ],
        compiler_params=pltpu.CompilerParams(
            collective_id=0, has_side_effects=True, vmem_limit_bytes=60 * 2**20
        ),
        name="relay_window",
    )(
        acts_fwd[0], grads_in[0], saved_acts[0], key_cotan[0], weight[0],
        gain, pos_fwd, pos_bwd, rate,
    )
    return keys[None], grad_out[None], weight_grad[None]


def solution(mesh):
    placed = (
        P("section", ("shard", "replica"), None),
        P("section", ("shard", "replica")),
        P("section", ("shard", "replica"), None),
        P("section", ("shard", "replica")),
        P("section", ("shard", "replica"), None),
        P("section", ("shard", "replica"), None),
        P("section", "shard", None),
        P("section", None),
    )
    return jax.shard_map(
        per_device,
        mesh=mesh,
        in_specs=placed,
        out_specs=(
            P("section", ("shard", "replica"), None),
            P("section", ("shard", "replica"), None),
            P("section", "shard", None),
        ),
        check_vma=False,
    )
```

```python
import functools

import jax
import jax.numpy as jnp
import numpy as np
from jax import lax
from jax.experimental import pallas as pl
from jax.experimental.pallas import tpu as pltpu
from jax.sharding import PartitionSpec as P

HEAD = 128
THETA = 500000.0
EPS = 1e-05
ROWS = 128
PARTS = 2
PIECES = 8
SKEW = 3
F32 = jnp.float32
BF16 = jnp.bfloat16
MESH = pl.DeviceIdType.MESH


def kernel(
    X, S, R,
    acts, grads, saved, kcot, w, gain, pos_f, pos_b, rate,
    keys_o, grad_o, wg_o,
    saved_v, kcot_v, w_v, stream_v, arrived_v,
    sv_recv, kg_all, st_recv, g_buf, g_send, p_buf, p_send, p_own,
    part, from_l, from_r, to_r, to_l, inv_v, tab_v,
    lsem, acts_ss, acts_rs, grads_sem, sv_ss, sv_rs, kg_ss, kg_rs,
    st_ss, st_rs, g_ss, g_rs, p_ss, p_rs, r_ss, r_rs, l_ss, l_rs,
):
    s, j, r = (lax.axis_index(a) for a in ("section", "shard", "replica"))
    T, D = saved.shape
    N = kcot.shape[1]
    Fs = w.shape[0]
    blocks = Fs // ROWS
    C = blocks * PARTS
    width = N // PARTS
    pieces = min(PIECES, blocks)
    Fp = Fs // pieces
    travel = to_r.dtype

    def cols(p, width=Fs, off=0):
        return pl.ds(pl.multiple_of(p * Fs + off, 128), width)

    def peer(d):
        return lax.rem(j + d, S)

    load_saved = pltpu.make_async_copy(saved, saved_v, lsem.at[0])
    load_kcot = pltpu.make_async_copy(kcot, kcot_v, lsem.at[1])
    load_w = pltpu.make_async_copy(w, w_v, lsem.at[2])
    load_acts = pltpu.make_async_copy(acts, stream_v, lsem.at[3])
    load_grads = pltpu.make_async_copy(grads, arrived_v, lsem.at[4])
    load_saved.start()
    load_kcot.start()
    load_w.start()
    pl.when(s == 0)(load_acts.start)
    pl.when(s == X - 1)(load_grads.start)

    barrier = pltpu.get_barrier_semaphore()

    def greet(axis, index):
        pl.semaphore_signal(barrier, inc=1, device_id={axis: index}, device_id_type=MESH)

    for d in range(1, S):
        greet("shard", peer(d))
    pl.when(s > 0)(lambda: greet("section", s - 1))
    pl.when(s < X - 1)(lambda: greet("section", s + 1))
    pl.when(r > 0)(lambda: greet("replica", r - 1))
    pl.when(r < R - 1)(lambda: greet("replica", r + 1))
    peers = S - 1
    for cond in (s > 0, s < X - 1, r > 0, r < R - 1):
        peers = peers + jnp.where(cond, 1, 0)
    pl.semaphore_wait(barrier, peers)

    def remote(src, dst, ss, rs, axis, index):
        return pltpu.make_async_remote_copy(
            src_ref=src, dst_ref=dst, send_sem=ss, recv_sem=rs,
            device_id={axis: index}, device_id_type=MESH,
        )

    def sv_copy(d, q):
        return remote(
            saved.at[:, cols(peer(d), Fp, q * Fp)],
            sv_recv.at[S - d, :, pl.ds(q * Fp, Fp)],
            sv_ss.at[d, q], sv_rs.at[S - d, q], "shard", peer(d),
        )

    def sv_wait(slot, q):
        remote(
            saved.at[:, pl.ds(0, Fp)],
            sv_recv.at[slot, :, pl.ds(pl.multiple_of(q * Fp, 128), Fp)],
            sv_ss.at[slot, q], sv_rs.at[slot, q], "shard", peer(slot),
        ).wait_recv()

    def slot_copy(src, dst, ss, rs, d):
        return remote(src.at[d], dst.at[S - d], ss.at[d], rs.at[S - d], "shard", peer(d))

    def slot_wait(src, dst, ss, rs, slot):
        remote(src.at[slot], dst.at[slot], ss.at[slot], rs.at[slot], "shard", peer(slot)).wait_recv()

    def acts_copy(d):
        return remote(
            acts.at[:, cols(peer(d))], stream_v.at[:, cols(peer(d))],
            acts_ss.at[d], acts_rs.at[d], "section", jnp.minimum(s + 1, X - 1),
        )

    grads_copy = remote(
        grads, arrived_v, grads_sem.at[0], grads_sem.at[1], "section", jnp.maximum(s - 1, 0)
    )

    def kg_copy(d):
        return remote(
            kg_all.at[0], kg_all.at[S - d], kg_ss.at[d], kg_rs.at[S - d], "shard", peer(d)
        )

    def st_copy(d):
        return remote(
            stream_v.at[:, cols(peer(d))], st_recv.at[S - d],
            st_ss.at[d], st_rs.at[S - d], "shard", peer(d),
        )

    def right_copy(c):
        return remote(
            to_r.at[c], from_l.at[c], r_ss.at[c], r_rs.at[c], "replica", jnp.minimum(r + 1, R - 1)
        )

    def left_copy(c):
        return remote(
            to_l.at[c], from_r.at[c], l_ss.at[c], l_rs.at[c], "replica", jnp.maximum(r - 1, 0)
        )

    for d in range(1, S):
        sv_copy(d, 0).start()

    @pl.when(s < X - 1)
    def _():
        for d in (*range(1, S), 0):
            acts_copy(d).start()

    @pl.when(s > 0)
    def _():
        grads_copy.start()

    lane = lax.broadcasted_iota(jnp.int32, (T, HEAD), 1)

    def tables(pos):
        angle = jnp.broadcast_to(pos[...].astype(F32), (T, T)).T[:, :1] * rate[...]
        sine = jnp.sin(angle)
        return jnp.cos(angle), jnp.where(lane < HEAD // 2, -sine, sine)

    def inverse_rms(ref):
        total = jnp.zeros((T, 128), F32)
        for c in range(D // 128):
            v = ref[:, c * 128 : (c + 1) * 128].astype(F32)
            total = total + v * v
        return lax.rsqrt(jnp.sum(total, -1, keepdims=True) / D + EPS)

    cos_b, sin_b = tables(pos_b)
    load_saved.wait()
    load_kcot.wait()
    inverse = inverse_rms(saved_v)
    inv_v[...] = jnp.broadcast_to(inverse, inv_v.shape)
    for h in range(N // HEAD):
        head = slice(h * HEAD, (h + 1) * HEAD)
        v = kcot_v[:, head].astype(F32)
        v = v * cos_b - pltpu.roll(v, HEAD // 2, 1) * sin_b
        kg_all[0, :, head] = (v * inverse).astype(BF16)
    for d in range(1, S):
        kg_copy(d).start()
    for q in range(1, pieces):
        for d in range(1, S):
            sv_copy(d, q).start()

    cos_f, sin_f = tables(pos_f)
    tab_v[0] = cos_f
    tab_v[1] = sin_f
    for d in range(1, S):
        slot_wait(kg_all, kg_all, kg_ss, kg_rs, d)

    def relay():
        pl.when(s == 0)(load_acts.wait)
        for d in range(1, S):
            pl.when(s > 0)(acts_copy(d).wait_recv)
            st_copy(d).start()

    tile = min(512, Fs)

    def backward():
        load_w.wait()

        @pl.loop(0, Fs // tile)
        def _(i):
            at = pl.ds(pl.multiple_of(i * tile, 128), tile)
            m = lax.dot_general(
                kg_all[...].reshape(S * T, N), w_v[at, :], (((1,), (1,)), ((), ())),
                preferred_element_type=F32,
            )
            m = (m * gain[:, cols(j, tile, i * tile)]).astype(BF16)
            g_buf[0, :, at] = m[:T]
            for d in range(1, S):
                g_send[d, :, at] = m[d * T : (d + 1) * T]

        for d in range(1, S):
            slot_copy(g_send, g_buf, g_ss, g_rs, d).start()

    def project(block):
        total = jnp.zeros((T, N), F32)
        for i in range(Fs // tile):
            g = gain[:, cols(j, tile, i * tile)]
            x = (block(i * tile).astype(F32) * g).astype(BF16)
            total = total + jnp.dot(
                x, w_v[i * tile : (i + 1) * tile, :], preferred_element_type=F32
            )
        return total

    def forward_own():
        pl.when(s > 0)(acts_copy(0).wait_recv)
        p_own[...] = project(lambda o: stream_v[:, cols(j, tile, o)])

    def forward_peers():
        for d in range(1, S):
            remote(
                stream_v.at[:, pl.ds(0, Fs)], st_recv.at[d], st_ss.at[d], st_rs.at[d],
                "shard", peer(d),
            ).wait_recv()
            p_send[d] = project(lambda o: st_recv[d, :, o : o + tile]).astype(p_send.dtype)
            slot_copy(p_send, p_buf, p_ss, p_rs, d).start()

    def finish_grad():
        pl.when(s == X - 1)(load_grads.wait)
        pl.when(s < X - 1)(grads_copy.wait_recv)
        for d in range(1, S):
            slot_wait(g_send, g_buf, g_ss, g_rs, d)
        total = jnp.zeros((T, 128), F32)
        for d in range(S):
            for o in range(0, Fs, 128):
                v = saved_v[:, cols(peer(d), 128, o)].astype(F32)
                total = total + v * g_buf[d, :, o : o + 128].astype(F32)
        inv = inv_v[:, :1]
        factor = inv * inv * (jnp.sum(total, -1, keepdims=True) / D)
        for d in range(S):
            for o in range(0, Fs, 128):
                at = cols(peer(d), 128, o)
                v = saved_v[:, at].astype(F32) * factor
                g = arrived_v[:, at].astype(F32) + g_buf[d, :, o : o + 128].astype(F32)
                grad_o[:, at] = (g - v).astype(BF16)

    def finish_keys():
        inv = inverse_rms(stream_v)
        for d in range(1, S):
            slot_wait(p_send, p_buf, p_ss, p_rs, d)
        for h in range(N // HEAD):
            head = slice(h * HEAD, (h + 1) * HEAD)
            v = p_own[:, head]
            for d in range(1, S):
                v = v + p_buf[d, :, head].astype(F32)
            v = v * inv
            v = v * tab_v[0] + pltpu.roll(v, HEAD // 2, 1) * tab_v[1]
            keys_o[:, head] = v.astype(BF16)

    scale = float(T * S * R) ** -0.5

    def when_chunk(c, *conds):
        cond = (c >= 0) & (c < C)
        for extra in conds:
            cond = cond & extra
        return pl.when(cond)

    far = SKEW * jnp.maximum(r, R - 1 - r)
    per_piece = C // pieces
    tasks = {2: relay, 4: backward, 8: forward_own, 14: forward_peers}
    steps = C + SKEW * (R - 1)

    def step(t, carry):
        @pl.when((t < C) & (lax.rem(t, per_piece) == 0))
        def _():
            for d in range(1, S):
                sv_wait(d, t // per_piece)

        @pl.when((t < C) & (lax.rem(t, PARTS) == 0))
        def _():
            o = (t // PARTS) * ROWS
            g = gain[:, cols(j, ROWS, o)]
            sides = [saved_v[:, cols(j, ROWS, o)]]
            for d in range(1, S):
                sides.append(sv_recv[d, :, pl.ds(pl.multiple_of(o, 128), ROWS)])
            x = jnp.concatenate([(v.astype(F32) * g).astype(BF16) for v in sides], 0)
            term = lax.dot_general(
                x, kg_all[...].reshape(S * T, N), (((0,), (0,)), ((), ())),
                preferred_element_type=F32,
            )
            for h in range(PARTS):
                part[t + h] = term[:, h * width : (h + 1) * width]

        a = t - SKEW * r

        @when_chunk(a, r == 0, r < R - 1)
        def _():
            to_r[a] = part[a].astype(travel)
            right_copy(a).start()

        @when_chunk(a, r > 0)
        def _():
            right_copy(a).wait_recv()

        @when_chunk(a, r > 0, r < R - 1)
        def _():
            to_r[a] = (part[a] + from_l[a].astype(F32)).astype(travel)
            right_copy(a).start()

        b = t - SKEW * (R - 1 - r)

        @when_chunk(b, r == R - 1, r > 0)
        def _():
            to_l[b] = part[b].astype(travel)
            left_copy(b).start()

        @when_chunk(b, r < R - 1)
        def _():
            left_copy(b).wait_recv()

        @when_chunk(b, r < R - 1, r > 0)
        def _():
            to_l[b] = (part[b] + from_r[b].astype(F32)).astype(travel)
            left_copy(b).start()

        f = t - far

        def finish(*sums):
            rows = pl.ds(pl.multiple_of((f // PARTS) * ROWS, ROWS), ROWS)
            at = pl.ds(pl.multiple_of(lax.rem(f, PARTS) * width, 128), width)
            total = part[f]
            for ref in sums:
                total = total + ref[f].astype(F32)
            wg_o[rows, at] = total * scale

        when_chunk(f, r == 0, r < R - 1)(lambda: finish(from_r))
        when_chunk(f, r > 0, r < R - 1)(lambda: finish(from_l, from_r))
        when_chunk(f, r > 0, r == R - 1)(lambda: finish(from_l))
        if R == 1:
            when_chunk(f)(finish)

        for at, task in tasks.items():
            pl.when(t == min(at, C - 1))(task)
        pl.when(t == min(26, steps - 1))(finish_grad)
        pl.when(t == min(30, steps - 1))(finish_keys)
        return carry

    lax.fori_loop(0, steps, step, 0)

    for d in range(1, S):
        for q in range(pieces):
            sv_copy(d, q).wait_send()
        kg_copy(d).wait_send()
        st_copy(d).wait_send()
        slot_copy(g_send, g_buf, g_ss, g_rs, d).wait_send()
        slot_copy(p_send, p_buf, p_ss, p_rs, d).wait_send()

    @pl.when(s < X - 1)
    def _():
        for d in range(S):
            acts_copy(d).wait_send()

    @pl.when(s > 0)
    def _():
        grads_copy.wait_send()

    @pl.loop(0, C)
    def _(c):
        pl.when(r < R - 1)(right_copy(c).wait_send)
        pl.when(r > 0)(left_copy(c).wait_send)


def store_kernel(a, b, c, a_out, b_out, c_out, sem):
    copies = [
        pltpu.make_async_copy(src, dst, sem.at[i])
        for i, (src, dst) in enumerate(((c, c_out), (b, b_out), (a, a_out)))
    ]
    for copy in copies:
        copy.start()
    for copy in copies:
        copy.wait()


def per_device(acts_fwd, pos_fwd, saved_acts, pos_bwd, grads_in, key_cotan, weight, gain):
    X, S, R = (lax.axis_size(a) for a in ("section", "shard", "replica"))
    T, D = acts_fwd.shape[1:]
    Fs, N = weight.shape[1:]
    C = Fs // ROWS * PARTS
    width = N // PARTS
    pieces = min(PIECES, Fs // ROWS)
    travel = BF16 if R <= 8 else F32
    index = np.arange(HEAD) % (HEAD // 2)
    rate = jnp.asarray(THETA ** (-(2.0 * index) / HEAD), F32)[None]
    hbm = pl.BlockSpec(memory_space=pltpu.HBM)
    vmem = pl.BlockSpec(memory_space=pltpu.VMEM)
    dma = pltpu.SemaphoreType.DMA
    results = pl.pallas_call(
        functools.partial(kernel, X, S, R),
        out_shape=(
            pltpu.VMEM((T, N), BF16),
            pltpu.VMEM((T, D), BF16),
            pltpu.VMEM((Fs, N), F32),
        ),
        in_specs=[hbm] * 5 + [vmem] * 4,
        out_specs=(vmem, vmem, vmem),
        scratch_shapes=[
            pltpu.VMEM((T, D), BF16),
            pltpu.VMEM((T, N), BF16),
            pltpu.VMEM((Fs, N), BF16),
            pltpu.VMEM((T, D), BF16),
            pltpu.VMEM((T, D), BF16),
            pltpu.VMEM((S, T, Fs), BF16),
            pltpu.VMEM((S, T, N), BF16),
            pltpu.VMEM((S, T, Fs), BF16),
            pltpu.VMEM((S, T, Fs), BF16),
            pltpu.VMEM((S, T, Fs), BF16),
            pltpu.VMEM((S, T, N), BF16),
            pltpu.VMEM((S, T, N), BF16),
            pltpu.VMEM((T, N), F32),
            pltpu.VMEM((C, ROWS, width), F32),
            pltpu.VMEM((C, ROWS, width), travel),
            pltpu.VMEM((C, ROWS, width), travel),
            pltpu.VMEM((C, ROWS, width), travel),
            pltpu.VMEM((C, ROWS, width), travel),
            pltpu.VMEM((T, HEAD), F32),
            pltpu.VMEM((2, T, HEAD), F32),
            dma((5,)),
            dma((S,)), dma((S,)), dma((2,)),
            dma((S, pieces)), dma((S, pieces)),
            dma((S,)), dma((S,)),
            dma((S,)), dma((S,)),
            dma((S,)), dma((S,)),
            dma((S,)), dma((S,)),
            dma((C,)), dma((C,)), dma((C,)), dma((C,)),
        ],
        compiler_params=pltpu.CompilerParams(
            collective_id=0, has_side_effects=True, vmem_limit_bytes=int(57.8 * 2**20)
        ),
        name="relay_window",
    )(
        acts_fwd[0], grads_in[0], saved_acts[0], key_cotan[0], weight[0],
        gain, pos_fwd, pos_bwd, rate,
    )
    keys, grad_out, weight_grad = pl.pallas_call(
        store_kernel,
        out_shape=tuple(jax.ShapeDtypeStruct(v.shape, v.dtype) for v in results),
        in_specs=[vmem] * 3,
        out_specs=[hbm] * 3,
        scratch_shapes=[dma((3,))],
        compiler_params=pltpu.CompilerParams(vmem_limit_bytes=8 * 2**20),
        name="store_results",
    )(*results)
    return keys[None], grad_out[None], weight_grad[None]


def solution(mesh):
    placed = (
        P("section", ("shard", "replica"), None),
        P("section", ("shard", "replica")),
        P("section", ("shard", "replica"), None),
        P("section", ("shard", "replica")),
        P("section", ("shard", "replica"), None),
        P("section", ("shard", "replica"), None),
        P("section", "shard", None),
        P("section", None),
    )
    return jax.shard_map(
        per_device,
        mesh=mesh,
        in_specs=placed,
        out_specs=(
            P("section", ("shard", "replica"), None),
            P("section", ("shard", "replica"), None),
            P("section", "shard", None),
        ),
        check_vma=False,
    )
```
